128 devices in a mesh: seq: 32 (over z, x, y_lo), tp: 4 (over y_hi, core).
Axes of the slice: x: 4, y: 4 (y_hi: 2, y_lo: 2; y = y_hi * 2 + y_lo), z: 4, core: 2. Of those that a mesh axis runs over, the one named last changes fastest.
Arguments:
- queries: bfloat16 [8192, 4096], P('seq', 'tp'), may hold values from -48 to 48, as said below
- key_rows: bfloat16 [8192, 512], P('seq', 'tp'), may hold values from -6 to 6, as said below
- value_rows: bfloat16 [8192, 512], P('seq', 'tp'), may hold values from -6 to 6
- projection: bfloat16 [4096, 8192], P('tp'), may hold values from -0.125 to 0.125
Outputs:
- attention_out: bfloat16 [8192, 8192], P('seq', 'tp')
The draws below stay inside these ranges and needn't reach their ends.
Inputs may be any that keep to these rules, and one draw needn't show every extreme that they name: `queries`: entries of order one; a few queries late in the prompt may align strongly with earlier keys and reach about 45. `key_rows`: entries of order one.
All inputs are finite; a program needn't handle non-finite values.
Results may differ from the reference program's by a relative error of at most 0.012.
Values may be sent and summed in bfloat16 or wider, within the bound.
No kernel may reach another device: no remote copies, remote signals or barrier semaphores. Data moves between devices by JAX's collectives and lax.ppermute only.
A program may use at most 64 MiB of HBM per device.

```python
import math
import jax
import jax.numpy as jnp
from jax import lax

D = 8192
HD = 128
GROUP = 8
KV_HEADS = 4
TOKENS = 8192
Q_HEADS = 32


def shared_draw(key):
    base_key = jax.random.fold_in(key, 7711)
    key_a, key_b = jax.random.split(base_key, 2)
    key_width = KV_HEADS * HD
    query_width = KV_HEADS * GROUP * HD
    key_mat = jnp.clip(jax.random.normal(key_a, (TOKENS, key_width), jnp.float32), -4.0, 4.0)
    query_mat = jnp.clip(jax.random.normal(key_b, (TOKENS, query_width), jnp.float32), -4.0, 4.0)
    return (query_mat, key_mat)


def draw_queries(key, part):
    query_mat, key_mat = shared_draw(key)
    return query_mat.astype(jnp.bfloat16)


def draw_key_rows(key, part):
    query_mat, key_mat = shared_draw(key)
    return key_mat.astype(jnp.bfloat16)


def strengthened(entries, key, source, target, parts, factor):
    def block_of(dim):
        return (jnp.arange(entries.shape[dim]) // (entries.shape[dim] // parts)).reshape((-1,) + (1,) * (entries.ndim - 1 - dim))

    one_side = jax.random.permutation(key, parts)[block_of(target)]
    other_side = (block_of(target) + parts // 2) % parts
    return jnp.where((block_of(source) == one_side) | (block_of(source) == other_side), factor * entries, entries)


def steps_of(rng, dims, shards, least, top_value):
    def one(axis_at, shards_of):
        steps = jax.random.uniform(jax.random.fold_in(jax.random.fold_in(rng, 6), axis_at), (shards_of,), jnp.float32, least / len(shards), top_value / len(shards))
        return jnp.repeat(jnp.exp(steps), dims[axis_at] // shards_of).reshape((-1,) + (1,) * (len(dims) - axis_at - 1))

    factor_of = one(*shards[0])
    for cut in shards[1:]:
        factor_of = factor_of * one(*cut)
    return factor_of


def noise(own_key, extent, scale, limit, pieces=(), held_as=jnp.bfloat16):
    entries = jax.random.normal(own_key, extent, jnp.float32) * scale
    if len(pieces) > 0:
        entries = steps_of(own_key, extent, pieces, -0.22, 0.18) * entries
    return jnp.clip(entries, min=-limit, max=limit).astype(held_as)


def bell_draw_with(stream_key, shape, scale, limit, cuts, heavy, held_as=jnp.bfloat16):
    drawn = scale * jax.random.normal(stream_key, shape, jnp.float32)
    if cuts:
        drawn = drawn * steps_of(stream_key, shape, cuts, -0.22, 0.18)
    return jnp.clip(strengthened(drawn, jax.random.fold_in(stream_key, 3), *heavy), -limit, limit).astype(held_as)


def setup_inputs(seed: int = 0) -> dict:
    keys = jax.random.split(jax.random.key(seed), 5)
    queries = draw_queries(jax.random.fold_in(keys[4], 71), 0)
    key_rows = draw_key_rows(jax.random.fold_in(keys[4], 71), 0)
    value_rows = noise(keys[2], (TOKENS, KV_HEADS * HD), 1.0, 6.0, ((0, 32), (1, 4)))
    projection = bell_draw_with(keys[3], (Q_HEADS * HD, D), (Q_HEADS * HD) ** -0.5, 0.125, ((0, 4),), (0, 1, 4, 2.0))
    return {"queries": queries, "key_rows": key_rows, "value_rows": value_rows, "projection": projection}


def reference(queries, key_rows, value_rows, projection):
    tok_count = queries.shape[0]
    q_block_rows = math.gcd(tok_count, 256)
    block_count = tok_count // q_block_rows
    scale = HD ** -0.5
    key_pos = jnp.arange(tok_count, dtype=jnp.int32)
    grand_total = jnp.zeros((tok_count, projection.shape[1]), jnp.float32)
    for group_id in range(KV_HEADS):
        key_mat = key_rows[:, group_id * HD:(group_id + 1) * HD]
        value_mat = value_rows[:, group_id * HD:(group_id + 1) * HD]
        width = GROUP * HD
        query_mat = queries[:, group_id * width:(group_id + 1) * width]
        stacked = query_mat.reshape(block_count, q_block_rows * GROUP, HD)

        def one_block(pair):
            q_block, block_id = pair
            scores = jnp.dot(q_block, key_mat.T, preferred_element_type=jnp.float32) * scale
            positions = block_id * q_block_rows + jnp.arange(q_block_rows * GROUP, dtype=jnp.int32) // GROUP
            scores = jnp.where(key_pos[None, :] <= positions[:, None], scores, -1e30)
            top_score = jnp.max(scores, axis=1)
            weights = jnp.exp(scores - top_score[:, None]).astype(jnp.bfloat16)
            totals = jnp.sum(weights.astype(jnp.float32), axis=1)
            mixed = jnp.dot(weights, value_mat, preferred_element_type=jnp.float32) / totals[:, None]
            return mixed.reshape(q_block_rows, width).astype(jnp.bfloat16)

        heads_out = lax.map(one_block, (stacked, jnp.arange(block_count, dtype=jnp.int32)))
        heads_out = heads_out.reshape(tok_count, width)
        partial_value = jnp.dot(heads_out, projection[group_id * width:(group_id + 1) * width], preferred_element_type=jnp.float32).astype(jnp.bfloat16)
        partial_value = lax.optimization_barrier(partial_value)
        grand_total = grand_total + partial_value.astype(jnp.float32)
    return grand_total.astype(jnp.bfloat16)
```

```python
import functools

import jax
import jax.numpy as jnp
from jax import lax
from jax.experimental import pallas as pl
from jax.experimental.pallas import tpu as pltpu
from jax.sharding import PartitionSpec as P

NZ, NX, NY, NH, NC = 4, 4, 2, 2, 2
AXES = ("seq", "tp")
STEPS = (1, 3, 2)
BLK = 256


def routes(move):
    def flat(z, x, y, h, c):
        return ((z * NX + x) * NY + y) * NH * NC + h * NC + c

    pairs = []
    for z in range(NZ):
        for x in range(NX):
            for y in range(NY):
                for h in range(NH):
                    for c in range(NC):
                        a, b, d, e, f = move(z, x, y, h, c)
                        pairs.append((flat(z, x, y, h, c), flat(a % NZ, b % NX, d % NY, e % NH, f % NC)))
    return pairs


def send(a, move):
    return lax.ppermute(a, AXES, routes(move))


def along_y(a):
    return send(a, lambda z, x, y, h, c: (z, x, y + 1, h, c))


def along_x(a, d):
    return send(a, lambda z, x, y, h, c: (z, x + d, y, h, c))


def along_z(a, d):
    return send(a, lambda z, x, y, h, c: (z + d, x, y, h, c))


def other_core(a):
    return send(a, lambda z, x, y, h, c: (z, x, y, h, c + 1))


def other_half(a):
    return send(a, lambda z, x, y, h, c: (z, x, y, h + 1, c))


def attend_kernel(place, q_ref, own, *rest, heads, scale):
    ax, bz, az, bx = rest[0:3], rest[3:6], rest[6:9], rest[9:12]
    out_ref, kv, top, acc, sems = rest[12:]
    rows = q_ref.shape[0]
    z, x, y = place[0], place[1], place[2]
    c1 = scale * 1.4426950408889634

    blocks = []
    for i, d in enumerate(STEPS):
        blocks.append((ax[i], 0, lax.rem(x - d + NX, NX) < x))
        blocks.append((bz[i], 0, lax.rem(z - d + NZ, NZ) < z))
    for i, d in enumerate(STEPS):
        for k in range(4):
            blocks.append((az[i], k, lax.rem(z - d + NZ, NZ) < z))
    for i, d in enumerate(STEPS):
        blocks.append((bx[i], 0, lax.rem(x - d + NX, NX) < x))
        for k, e in enumerate(STEPS):
            blocks.append((bx[i], k + 1, lax.rem(z - e + NZ, NZ) < z))

    copies = []
    slot = jnp.int32(0)
    for i, (ref, k, needed) in enumerate(blocks):
        cp = pltpu.make_async_copy(
            ref.at[pl.ds(k * BLK, BLK)], kv.at[pl.ds(pl.multiple_of(slot * BLK, BLK), BLK)], sems.at[i]
        )
        copies.append((cp, needed))
        pl.when(needed)(cp.start)
        slot = slot + needed.astype(jnp.int32)

    top[...] = jnp.full(top.shape, -1e30, jnp.float32)
    acc[...] = jnp.zeros(acc.shape, jnp.float32)

    def fold(tile, valid):
        keys = tile.shape[0]
        key_mat = tile[:, :128]
        value_mat = jnp.concatenate([tile[:, 128:], jnp.ones((keys, 128), jnp.bfloat16)], axis=1)
        for h in range(heads):
            q = q_ref[:, h * 128 : (h + 1) * 128]
            s = lax.dot_general(q, key_mat, (((1,), (1,)), ((), ())), preferred_element_type=jnp.float32)
            if valid is not None:
                s = jnp.where(valid, s, -1e30)
            old = top[h]
            new = jnp.maximum(old, jnp.max(s, axis=1, keepdims=True))
            top[h] = new
            factor = jnp.exp2((old - new) * c1)
            base = new * c1
            p = jnp.exp2(s * c1 - jnp.concatenate([base] * (keys // 128), axis=1)).astype(jnp.bfloat16)
            pv = jnp.dot(p, value_mat, preferred_element_type=jnp.float32)
            acc[h] = acc[h] * jnp.concatenate([factor, factor], axis=1) + pv

    r = lax.broadcasted_iota(jnp.int32, (rows, 512), 0)
    k = lax.broadcasted_iota(jnp.int32, (rows, 512), 1)
    side = lax.rem(lax.div(k, 128), 2)
    off = lax.div(k, 256) * 128 + lax.rem(k, 128)
    valid = jnp.where(side == 0, off, off + jnp.where(y == 0, 256, -256)) <= r
    fold(own[...], valid)

    for cp, needed in copies:
        pl.when(needed)(cp.wait)

    def step(g, carry):
        fold(kv[pl.ds(pl.multiple_of(g * 1024, 1024), 1024), :], None)
        return carry

    pairs = lax.div(slot, 4)
    lax.fori_loop(0, pairs, step, 0)

    @pl.when(lax.rem(slot, 4) > 0)
    def _():
        fold(kv[pl.ds(pl.multiple_of(pairs * 1024, 1024), 512), :], None)

    for h in range(heads):
        a = acc[h]
        out_ref[:, h * 128 : (h + 1) * 128] = (a[:, :128] / a[:, 128:]).astype(jnp.bfloat16)


def attend(place, queries, own, others):
    rows, width = queries.shape
    heads = width // 128
    vm = pl.BlockSpec(memory_space=pltpu.VMEM)
    hbm = pl.BlockSpec(memory_space=pl.ANY)
    return pl.pallas_call(
        functools.partial(attend_kernel, heads=heads, scale=128 ** -0.5),
        out_shape=jax.ShapeDtypeStruct((rows, width), jnp.bfloat16),
        in_specs=[pl.BlockSpec(memory_space=pltpu.SMEM), vm, vm] + [hbm] * len(others),
        out_specs=vm,
        scratch_shapes=[
            pltpu.VMEM((32 * BLK, 256), jnp.bfloat16),
            pltpu.VMEM((heads, rows, 128), jnp.float32),
            pltpu.VMEM((heads, rows, 256), jnp.float32),
            pltpu.SemaphoreType.DMA((30,)),
        ],
        cost_estimate=pl.CostEstimate(flops=4 * 8192 * 2048 * 128, bytes_accessed=8 << 20, transcendentals=8192 * 2048),
        name="attend",
    )(place, queries, own, *others)


def project_kernel(col, heads_ref, w_ref, *rest):
    out = jnp.dot(heads_ref[...], w_ref[...], preferred_element_type=jnp.float32)
    if len(rest) == 2:
        out = out + rest[0][...].astype(jnp.float32)
    rest[-1][...] = out.astype(rest[-1].dtype)


def project(heads_out, projection, col, plus=None, dtype=jnp.bfloat16):
    rows, depth = heads_out.shape
    cols, tile = 2048, 512
    steps = cols // tile
    extra = [] if plus is None else [plus]
    return pl.pallas_call(
        project_kernel,
        out_shape=jax.ShapeDtypeStruct((rows, cols), dtype),
        grid_spec=pltpu.PrefetchScalarGridSpec(
            num_scalar_prefetch=1,
            grid=(steps,),
            in_specs=[
                pl.BlockSpec((rows, depth), lambda i, c: (0, 0)),
                pl.BlockSpec((depth, tile), lambda i, c: (0, c[0] * steps + i)),
            ]
            + [pl.BlockSpec((rows, tile), lambda i, c: (0, i))] * len(extra),
            out_specs=pl.BlockSpec((rows, tile), lambda i, c: (0, i)),
        ),
        cost_estimate=pl.CostEstimate(flops=2 * rows * depth * cols, bytes_accessed=6 << 20, transcendentals=0),
        name="project",
    )(col, heads_out, projection, *extra)


def on_device(queries, key_rows, value_rows, projection):
    seq = lax.axis_index("seq")
    tp = lax.axis_index("tp")
    place = jnp.stack([seq // (NX * NY), (seq // NY) % NX, seq % NY]).astype(jnp.int32)

    both = jnp.concatenate([key_rows, value_rows], axis=1)
    near = along_y(both)
    pair_a = jnp.concatenate([both[:128], near[:128]], axis=0)
    pair_b = jnp.concatenate([both[128:], near[128:]], axis=0)
    own = jnp.concatenate([pair_a, pair_b], axis=0)
    ax = [along_x(pair_a, d) for d in STEPS]
    bz = [along_z(pair_b, d) for d in STEPS]
    all_a = jnp.concatenate([pair_a] + ax, axis=0)
    all_b = jnp.concatenate([pair_b] + bz, axis=0)
    az = [along_z(all_a, d) for d in STEPS]
    bx = [along_x(all_b, d) for d in STEPS]

    heads_out = attend(place, queries, own, ax + bz + az + bx)

    def part(flip):
        return (tp ^ flip).astype(jnp.int32).reshape(1)

    far = project(heads_out, projection, part(3))
    far = other_core(far)
    side = project(heads_out, projection, part(1))
    side = other_core(side)
    cross = project(heads_out, projection, part(2), far)
    cross = other_half(cross)
    mine = project(heads_out, projection, part(0), side, jnp.float32)
    return (mine + cross.astype(jnp.float32)).astype(jnp.bfloat16)


def solution(mesh):
    in_specs = (P("seq", "tp"), P("seq", "tp"), P("seq", "tp"), P("tp", None))
    return jax.shard_map(on_device, mesh=mesh, in_specs=in_specs, out_specs=P("seq", "tp"), check_vma=False)
```

```python
import functools

import jax
import jax.numpy as jnp
from jax import lax
from jax.experimental import pallas as pl
from jax.experimental.pallas import tpu as pltpu
from jax.sharding import PartitionSpec as P

NZ, NX, NY, NH, NC = 4, 4, 2, 2, 2
AXES = ("seq", "tp")
KEYS = 512
HD = 128
UNIT = HD**-0.5 * 1.4426950408889634
LIMIT = 60.0

ROUNDS = (
    (((-1, 0), (0, 0), (1, 0)), ((1, 0), (0, 0), (-1, 0)), ((0, -1), (0, 0), (0, 1)), ((0, 1), (0, 0), (0, -1))),
    (((2, 0), (-1, 0), (1, 0)), ((1, 1), (0, 1), (-1, 0)), ((-1, -1), (-1, 0), (0, 1)), ((0, 2), (0, 1), (0, -1))),
    (((-1, 1), (0, 1), (1, 0)), ((1, -1), (0, -1), (-1, 0)), ((2, -1), (2, 0), (0, 1)), ((2, 1), (2, 0), (0, -1))),
    (((-1, 2), (0, 2), (1, 0)), ((1, 2), (0, 2), (-1, 0)), ((2, 2), (2, 1), (0, -1))),
)


def flat(z, x, y, h, c):
    return ((z * NX + x) * NY + y) * NH * NC + h * NC + c


def send(a, move, keep=lambda z, x: True):
    pairs = []
    for z in range(NZ):
        for x in range(NX):
            for y in range(NY):
                for h in range(NH):
                    for c in range(NC):
                        tz, tx, ty, th, tc = move(z, x, y, h, c)
                        tz, tx, ty, th, tc = tz % NZ, tx % NX, ty % NY, th % NH, tc % NC
                        if keep(tz, tx):
                            pairs.append((flat(z, x, y, h, c), flat(tz, tx, ty, th, tc)))
    return lax.ppermute(a, AXES, pairs)


def wanted(offset, z, x):
    source = ((z + offset[1]) % NZ, (x + offset[0]) % NX)
    if source < (z, x):
        return True
    for hops in ROUNDS:
        for later, parent, (dx, dz) in hops:
            if parent == offset and parent != (0, 0) and wanted(later, (z + dz) % NZ, (x + dx) % NX):
                return True
    return False


def exact_fold(h, q_ref, tile, valid, top, acc):
    keys = tile.shape[0]
    q = q_ref[:, pl.ds(pl.multiple_of(h * HD, HD), HD)]
    s = lax.dot_general(q, tile[:, :HD], (((1,), (1,)), ((), ())), preferred_element_type=jnp.float32)
    u = s * UNIT
    if valid is not None:
        u = jnp.where(valid, u, -1e30)
    old = top[h]
    new = jnp.maximum(old, jnp.max(u, axis=1, keepdims=True))
    top[h] = new
    factor = jnp.exp2(old - new)
    p = jnp.exp2(u - jnp.concatenate([new] * (keys // HD), axis=1)).astype(jnp.bfloat16)
    value_mat = jnp.concatenate([tile[:, HD:], jnp.ones((keys, HD), jnp.bfloat16)], axis=1)
    acc[h] = acc[h] * jnp.concatenate([factor, factor], axis=1) + jnp.dot(
        p, value_mat, preferred_element_type=jnp.float32
    )


def fast_fold(q_ref, tile, top, acc, worst):
    keys = tile.shape[0]
    rows = q_ref.shape[0]
    value_mat = jnp.concatenate([tile[:, HD:], jnp.ones((keys, HD), jnp.bfloat16)], axis=1)
    for h in range(acc.shape[0]):
        q = q_ref[:, h * HD : (h + 1) * HD]
        s = lax.dot_general(q, tile[:, :HD], (((1,), (1,)), ((), ())), preferred_element_type=jnp.float32)
        u = s * UNIT - jnp.concatenate([top[h]] * (keys // HD), axis=1)
        high = u[:, :HD]
        for j in range(1, keys // HD):
            high = jnp.maximum(high, u[:, j * HD : (j + 1) * HD])
        p = jnp.exp2(u).astype(jnp.bfloat16)
        acc[h] = acc[h] + jnp.dot(p, value_mat, preferred_element_type=jnp.float32)
        worst = jnp.maximum(worst, jnp.max(high.reshape(rows // 8, 8, HD), axis=0))
    return worst


def first_kernel(place, q_ref, own, top, acc):
    rows = q_ref.shape[0]
    top[...] = jnp.full(top.shape, -1e30, jnp.float32)
    acc[...] = jnp.zeros(acc.shape, jnp.float32)
    r = lax.broadcasted_iota(jnp.int32, (rows, KEYS), 0)
    k = lax.broadcasted_iota(jnp.int32, (rows, KEYS), 1)
    valid = jnp.where(k < 256, k, k + jnp.where(place[2] == 0, 0, -512)) <= r

    def head(h, carry):
        exact_fold(h, q_ref, own[...], valid, top, acc)
        return carry

    lax.fori_loop(0, acc.shape[0], head, 0, unroll=4)


def step_kernel(place, q_ref, top_in, acc_in, *rest, offsets, last):
    n = len(offsets)
    blocks, rest = rest[:n], rest[n:]
    if last:
        w_ref, heads_ref, x_ref, held, top, acc, w_buf, sems = rest
        copies = load_columns(w_ref, place[3], w_buf, sems)
    else:
        top, acc, held = rest
    z, x = place[0], place[1]
    count = jnp.int32(0)
    for block, (dx, dz) in zip(blocks, offsets):
        sz, sx = lax.rem(z + dz + NZ, NZ), lax.rem(x + dx + NX, NX)
        needed = sz * NX + sx < z * NX + x

        @pl.when(needed)
        def _(block=block, at=count):
            held[pl.ds(pl.multiple_of(at * KEYS, KEYS), KEYS), :] = block[...]

        count = count + needed.astype(jnp.int32)

    top[...] = top_in[...]
    acc[...] = acc_in[...]

    def block_at(i):
        return held[pl.ds(pl.multiple_of(i * KEYS, KEYS), KEYS), :]

    worst = lax.fori_loop(
        0,
        count,
        lambda i, w: fast_fold(q_ref, block_at(i), top, acc, w),
        jnp.full((8, HD), -1e30, jnp.float32),
    )

    @pl.when(jnp.max(worst) > LIMIT)
    def _():
        acc[...] = acc_in[...]

        def again(i, carry):
            def head(h, c):
                exact_fold(h, q_ref, block_at(i), None, top, acc)
                return c

            return lax.fori_loop(0, acc.shape[0], head, carry)

        lax.fori_loop(0, count, again, 0)

    if last:
        for h in range(acc.shape[0]):
            a = acc[h]
            heads_ref[:, h * HD : (h + 1) * HD] = (a[:, :HD] / a[:, HD:]).astype(jnp.bfloat16)
        multiply_columns(heads_ref, w_buf, copies, x_ref)


WIDTH, CHUNK = 2048, 512


def load_columns(w_ref, part, w_buf, sems):
    copies = []
    for j in range(WIDTH // CHUNK):
        at = pl.multiple_of(part * WIDTH + j * CHUNK, CHUNK)
        copies.append(
            pltpu.make_async_copy(w_ref.at[:, pl.ds(at, CHUNK)], w_buf.at[:, pl.ds(j * CHUNK, CHUNK)], sems.at[j])
        )
        copies[-1].start()
    return copies


def multiply_columns(heads_ref, w_buf, copies, out_ref):
    for j, copy in enumerate(copies):
        copy.wait()
        out_ref[:, j * CHUNK : (j + 1) * CHUNK] = jnp.dot(
            heads_ref[...], w_buf[:, j * CHUNK : (j + 1) * CHUNK], preferred_element_type=jnp.float32
        ).astype(out_ref.dtype)


def project_kernel(part, heads_ref, w_ref, out_ref, w_buf, sems):
    multiply_columns(heads_ref, w_buf, load_columns(w_ref, part[0], w_buf, sems), out_ref)


SMEM = pl.BlockSpec(memory_space=pltpu.SMEM)
VMEM = pl.BlockSpec(memory_space=pltpu.VMEM)
HBM = pl.BlockSpec(memory_space=pltpu.HBM)
W_SCRATCH = [pltpu.VMEM((1024, WIDTH), jnp.bfloat16), pltpu.SemaphoreType.DMA((WIDTH // CHUNK,))]


def cost(blocks, mib):
    n = blocks * KEYS * 2048
    return pl.CostEstimate(flops=4 * n * HD, bytes_accessed=mib << 20, transcendentals=n)


def state_of(rows, heads):
    return (
        jax.ShapeDtypeStruct((heads, rows, HD), jnp.float32),
        jax.ShapeDtypeStruct((heads, rows, 2 * HD), jnp.float32),
    )


def attend_first(place, queries, own):
    rows, width = queries.shape
    return pl.pallas_call(
        first_kernel,
        out_shape=state_of(rows, width // HD),
        in_specs=[SMEM, VMEM, VMEM],
        out_specs=(VMEM, VMEM),
        compiler_params=pltpu.CompilerParams(vmem_limit_bytes=16 << 20),
        cost_estimate=cost(1, 4),
        name="attend_first",
    )(place, queries, own)


def attend_step(place, queries, state, offsets, blocks):
    rows, width = queries.shape
    return pl.pallas_call(
        functools.partial(step_kernel, offsets=offsets, last=False),
        out_shape=state_of(rows, width // HD),
        in_specs=[SMEM, VMEM, VMEM, VMEM] + [VMEM] * len(blocks),
        out_specs=(VMEM, VMEM),
        scratch_shapes=[pltpu.VMEM((len(blocks) * KEYS, 2 * HD), jnp.bfloat16)],
        compiler_params=pltpu.CompilerParams(vmem_limit_bytes=20 << 20),
        cost_estimate=cost(len(blocks), 4),
        name="attend_step",
    )(place, queries, *state, *blocks)


def attend_last(place, queries, state, offsets, blocks, projection):
    rows, width = queries.shape
    return pl.pallas_call(
        functools.partial(step_kernel, offsets=offsets, last=True),
        out_shape=(
            jax.ShapeDtypeStruct((rows, width), jnp.bfloat16),
            jax.ShapeDtypeStruct((rows, WIDTH), jnp.bfloat16),
        ),
        in_specs=[SMEM, VMEM, VMEM, VMEM] + [VMEM] * len(blocks) + [HBM],
        out_specs=(VMEM, VMEM),
        scratch_shapes=[pltpu.VMEM((len(blocks) * KEYS, 2 * HD), jnp.bfloat16)]
        + [pltpu.VMEM(s.shape, s.dtype) for s in state_of(rows, width // HD)]
        + W_SCRATCH,
        compiler_params=pltpu.CompilerParams(vmem_limit_bytes=50 << 20),
        cost_estimate=cost(len(blocks), 8),
        name="attend_last",
    )(place, queries, *state, *blocks, projection)


def project(heads_out, projection, part):
    rows = heads_out.shape[0]
    return pl.pallas_call(
        project_kernel,
        out_shape=jax.ShapeDtypeStruct((rows, WIDTH), jnp.bfloat16),
        in_specs=[SMEM, VMEM, HBM],
        out_specs=VMEM,
        scratch_shapes=W_SCRATCH,
        compiler_params=pltpu.CompilerParams(vmem_limit_bytes=50 << 20),
        cost_estimate=pl.CostEstimate(flops=2 * rows * 1024 * WIDTH, bytes_accessed=6 << 20, transcendentals=0),
        name="project",
    )(part.reshape(1), heads_out, projection)


def add(a, b):
    return (a.astype(jnp.float32) + b.astype(jnp.float32)).astype(jnp.bfloat16)


def on_device(queries, key_rows, value_rows, projection):
    seq = lax.axis_index("seq").astype(jnp.int32)
    tp = lax.axis_index("tp").astype(jnp.int32)
    place = jnp.stack([seq // (NX * NY), (seq // NY) % NX, seq % NY, tp ^ 3])

    both = jnp.concatenate([key_rows, value_rows], axis=1)
    near = send(both, lambda z, x, y, h, c: (z, x, y + 1, h, c))
    known = {(0, 0): jnp.concatenate([both, near], axis=0)}

    state = None
    pending = []
    for hops in ROUNDS:
        arrived = {}
        for offset, parent, (dx, dz) in hops:
            arrived[offset] = send(
                known[parent],
                lambda z, x, y, h, c, dx=dx, dz=dz: (z + dz, x + dx, y, h, c),
                lambda z, x, offset=offset: wanted(offset, z, x),
            )
        if state is None:
            state = attend_first(place, queries, known[(0, 0)])
        else:
            state = attend_step(place, queries, state, pending, [known[o] for o in pending])
        arrived, state = lax.optimization_barrier((arrived, state))
        known.update(arrived)
        pending = list(arrived)
    heads_out, far = attend_last(place, queries, state, pending, [known[o] for o in pending], projection)

    far = send(far, lambda z, x, y, h, c: (z, x, y, h, c + 1))
    cross = add(project(heads_out, projection, tp ^ 2), far)
    cross = send(cross, lambda z, x, y, h, c: (z, x, y, h + 1, c))
    side = send(project(heads_out, projection, tp ^ 1), lambda z, x, y, h, c: (z, x, y, h, c + 1))
    mine = project(heads_out, projection, tp)
    total = mine.astype(jnp.float32) + side.astype(jnp.float32) + cross.astype(jnp.float32)
    return total.astype(jnp.bfloat16)


def solution(mesh):
    in_specs = (P("seq", "tp"), P("seq", "tp"), P("seq", "tp"), P("tp", None))
    return jax.shard_map(on_device, mesh=mesh, in_specs=in_specs, out_specs=P("seq", "tp"), check_vma=False)
```

```python
import functools

import jax
import jax.numpy as jnp
from jax import lax
from jax.experimental import pallas as pl
from jax.experimental.pallas import tpu as pltpu
from jax.sharding import PartitionSpec as P

NZ, NX, NY, NH, NC = 4, 4, 2, 2, 2
AXES = ("seq", "tp")
HD = 128
UNIT = HD**-0.5 * 1.4426950408889634
LIMIT = 60.0

STEPS = (1, 3, 2)
BLK = 256


def flat(z, x, y, h, c):
    return ((z * NX + x) * NY + y) * NH * NC + h * NC + c


def send(a, move):
    pairs = []
    for z in range(NZ):
        for x in range(NX):
            for y in range(NY):
                for h in range(NH):
                    for c in range(NC):
                        tz, tx, ty, th, tc = move(z, x, y, h, c)
                        tz, tx, ty, th, tc = tz % NZ, tx % NX, ty % NY, th % NH, tc % NC
                        pairs.append((flat(z, x, y, h, c), flat(tz, tx, ty, th, tc)))
    return lax.ppermute(a, AXES, pairs)


def along_x(a, d):
    return send(a, lambda z, x, y, h, c: (z, x + d, y, h, c))


def along_z(a, d):
    return send(a, lambda z, x, y, h, c: (z + d, x, y, h, c))


def exact_fold(h, q_ref, tile, valid, top, acc):
    keys = tile.shape[0]
    q = q_ref[:, pl.ds(pl.multiple_of(h * HD, HD), HD)]
    s = lax.dot_general(q, tile[:, :HD], (((1,), (1,)), ((), ())), preferred_element_type=jnp.float32)
    u = s * UNIT
    if valid is not None:
        u = jnp.where(valid, u, -1e30)
    old = top[h]
    new = jnp.maximum(old, jnp.max(u, axis=1, keepdims=True))
    top[h] = new
    factor = jnp.exp2(old - new)
    p = jnp.exp2(u - jnp.concatenate([new] * (keys // HD), axis=1)).astype(jnp.bfloat16)
    value_mat = jnp.concatenate([tile[:, HD:], jnp.ones((keys, HD), jnp.bfloat16)], axis=1)
    acc[h] = acc[h] * jnp.concatenate([factor, factor], axis=1) + jnp.dot(
        p, value_mat, preferred_element_type=jnp.float32
    )


def fast_fold(q_ref, tile, top, acc, worst):
    keys = tile.shape[0]
    rows = q_ref.shape[0]
    value_mat = jnp.concatenate([tile[:, HD:], jnp.ones((keys, HD), jnp.bfloat16)], axis=1)
    for h in range(acc.shape[0]):
        q = q_ref[:, h * HD : (h + 1) * HD]
        s = lax.dot_general(q, tile[:, :HD], (((1,), (1,)), ((), ())), preferred_element_type=jnp.float32)
        u = s * UNIT - jnp.concatenate([top[h]] * (keys // HD), axis=1)
        high = u[:, :HD]
        for j in range(1, keys // HD):
            high = jnp.maximum(high, u[:, j * HD : (j + 1) * HD])
        p = jnp.exp2(u).astype(jnp.bfloat16)
        acc[h] = acc[h] + jnp.dot(p, value_mat, preferred_element_type=jnp.float32)
        worst = jnp.maximum(worst, jnp.max(high.reshape(rows // 8, 8, HD), axis=0))
    return worst


def fold_own(q_ref, own, y, top, acc):
    rows = q_ref.shape[0]
    top[...] = jnp.full(top.shape, -1e30, jnp.float32)
    acc[...] = jnp.zeros(acc.shape, jnp.float32)
    r = lax.broadcasted_iota(jnp.int32, (rows, 2 * BLK), 0)
    k = lax.broadcasted_iota(jnp.int32, (rows, 2 * BLK), 1)
    position = lax.div(k, 256) * 128 + lax.rem(k, 128)
    position = position + jnp.where(lax.rem(lax.div(k, 128), 2) == 0, 0, jnp.where(y == 0, 256, -256))
    valid = position <= r

    def head(h, carry):
        exact_fold(h, q_ref, own[...], valid, top, acc)
        return carry

    lax.fori_loop(0, acc.shape[0], head, 0, unroll=4)


def step_kernel(place, q_ref, *rest, first, last, blocks):
    if first:
        own, rest = rest[0], rest[1:]
    else:
        top_in, acc_in, rest = rest[0], rest[1], rest[2:]
    n = len(blocks)
    refs, rest = rest[:n], rest[n:]
    if last:
        w_ref, heads_ref, x_ref, held, top, acc, w_buf, sems = rest
        copies = load_columns(w_ref, place[3], w_buf, sems)
    elif first:
        top, acc, held, top_in, acc_in = rest
    else:
        top, acc, held = rest
    z, x = place[0], place[1]
    count = jnp.int32(0)
    for ref, sources in zip(refs, blocks):
        for i, (dx, dz) in enumerate(sources):
            needed = lax.rem(z + dz, NZ) * NX + lax.rem(x + dx, NX) < z * NX + x

            @pl.when(needed)
            def _(ref=ref, i=i, at=count):
                held[pl.ds(pl.multiple_of(at * BLK, BLK), BLK), :] = ref[i * BLK : (i + 1) * BLK, :]

            count = count + needed.astype(jnp.int32)

    if first:
        fold_own(q_ref, own, place[2], top, acc)
        top_in[...] = top[...]
        acc_in[...] = acc[...]
    else:
        top[...] = top_in[...]
        acc[...] = acc_in[...]

    def keys_at(i, n):
        return held[pl.ds(pl.multiple_of(i * n, n), n), :]

    def odd(w):
        return fast_fold(q_ref, keys_at(count - 1, BLK), top, acc, w)

    worst = lax.fori_loop(
        0,
        lax.div(count, 2),
        lambda i, w: fast_fold(q_ref, keys_at(i, 2 * BLK), top, acc, w),
        jnp.full((8, HD), -1e30, jnp.float32),
    )
    worst = lax.cond(lax.rem(count, 2) == 1, odd, lambda w: w, worst)

    @pl.when(jnp.max(worst) > LIMIT)
    def _():
        acc[...] = acc_in[...]

        def again(i, carry):
            def head(h, c):
                exact_fold(h, q_ref, keys_at(i, BLK), None, top, acc)
                return c

            return lax.fori_loop(0, acc.shape[0], head, carry)

        lax.fori_loop(0, count, again, 0)

    if last:
        for h in range(acc.shape[0]):
            a = acc[h]
            heads_ref[:, h * HD : (h + 1) * HD] = (a[:, :HD] / a[:, HD:]).astype(jnp.bfloat16)
        multiply_columns(heads_ref, w_buf, copies, x_ref)


WIDTH, CHUNK = 2048, 512


def load_columns(w_ref, part, w_buf, sems):
    copies = []
    for j in range(WIDTH // CHUNK):
        at = pl.multiple_of(part * WIDTH + j * CHUNK, CHUNK)
        copies.append(
            pltpu.make_async_copy(w_ref.at[:, pl.ds(at, CHUNK)], w_buf.at[:, pl.ds(j * CHUNK, CHUNK)], sems.at[j])
        )
        copies[-1].start()
    return copies


def multiply_columns(heads_ref, w_buf, copies, out_ref):
    for j, copy in enumerate(copies):
        copy.wait()
        out_ref[:, j * CHUNK : (j + 1) * CHUNK] = jnp.dot(
            heads_ref[...], w_buf[:, j * CHUNK : (j + 1) * CHUNK], preferred_element_type=jnp.float32
        ).astype(out_ref.dtype)


def project_kernel(part, heads_ref, w_ref, out_ref, w_buf, sems):
    multiply_columns(heads_ref, w_buf, load_columns(w_ref, part[0], w_buf, sems), out_ref)


SMEM = pl.BlockSpec(memory_space=pltpu.SMEM)
VMEM = pl.BlockSpec(memory_space=pltpu.VMEM)
HBM = pl.BlockSpec(memory_space=pltpu.HBM)
W_SCRATCH = [pltpu.VMEM((1024, WIDTH), jnp.bfloat16), pltpu.SemaphoreType.DMA((WIDTH // CHUNK,))]


def cost(blocks, mib):
    n = blocks * 512 * 2048
    return pl.CostEstimate(flops=4 * n * HD, bytes_accessed=mib << 20, transcendentals=n)


def state_of(rows, heads):
    return (
        jax.ShapeDtypeStruct((heads, rows, HD), jnp.float32),
        jax.ShapeDtypeStruct((heads, rows, 2 * HD), jnp.float32),
    )


def attend(place, queries, state, own, operands, projection=None):
    arrays, blocks = [a for a, _ in operands], [b for _, b in operands]
    rows, width = queries.shape
    first, last = own is not None, projection is not None
    shapes = state_of(rows, width // HD)
    in_state = [own] if first else list(state)
    held = [pltpu.VMEM((sum(len(b) for b in blocks) * BLK, 2 * HD), jnp.bfloat16)]
    buffers = [pltpu.VMEM(s.shape, s.dtype) for s in shapes]
    out = (jax.ShapeDtypeStruct((rows, width), jnp.bfloat16), jax.ShapeDtypeStruct((rows, WIDTH), jnp.bfloat16))
    return pl.pallas_call(
        functools.partial(step_kernel, first=first, last=last, blocks=blocks),
        out_shape=out if last else shapes,
        in_specs=[SMEM, VMEM] + [VMEM] * (len(in_state) + len(arrays)) + [HBM] * last,
        out_specs=(VMEM, VMEM),
        scratch_shapes=held + (buffers + W_SCRATCH if last else buffers if first else []),
        compiler_params=pltpu.CompilerParams(vmem_limit_bytes=(45 if last else 20) << 20),
        cost_estimate=cost(4 + first, 8),
        name="attend_last" if last else "attend_first" if first else "attend_step",
    )(place, queries, *in_state, *arrays, *([projection] if last else []))


def pack_kernel(k_ref, v_ref, out_ref):
    out_ref[:, :HD] = k_ref[...]
    out_ref[:, HD:] = v_ref[...]


def pack(key_rows, value_rows):
    return pl.pallas_call(
        pack_kernel,
        out_shape=jax.ShapeDtypeStruct((key_rows.shape[0], 2 * HD), jnp.bfloat16),
        in_specs=[VMEM, VMEM],
        out_specs=VMEM,
        compiler_params=pltpu.CompilerParams(vmem_limit_bytes=4 << 20),
        name="pack",
    )(key_rows, value_rows)


def project(heads_out, projection, part):
    rows = heads_out.shape[0]
    return pl.pallas_call(
        project_kernel,
        out_shape=jax.ShapeDtypeStruct((rows, WIDTH), jnp.bfloat16),
        in_specs=[SMEM, VMEM, HBM],
        out_specs=VMEM,
        scratch_shapes=W_SCRATCH,
        compiler_params=pltpu.CompilerParams(vmem_limit_bytes=50 << 20),
        cost_estimate=pl.CostEstimate(flops=2 * rows * 1024 * WIDTH, bytes_accessed=6 << 20, transcendentals=0),
        name="project",
    )(part.reshape(1), heads_out, projection)


def add(a, b):
    return (a.astype(jnp.float32) + b.astype(jnp.float32)).astype(jnp.bfloat16)


def on_device(queries, key_rows, value_rows, projection):
    seq = lax.axis_index("seq").astype(jnp.int32)
    tp = lax.axis_index("tp").astype(jnp.int32)
    place = jnp.stack([seq // (NX * NY), (seq // NY) % NX, seq % NY, tp ^ 3])

    both = pack(key_rows, value_rows)
    near = send(both, lambda z, x, y, h, c: (z, x, y + 1, h, c))
    pair_a = jnp.concatenate([both[:128], near[:128]], axis=0)
    pair_b = jnp.concatenate([both[128:], near[128:]], axis=0)
    own = jnp.concatenate([pair_a, pair_b], axis=0)
    ax = [along_x(pair_a, d) for d in STEPS]
    bz = [along_z(pair_b, d) for d in STEPS]
    all_a = jnp.concatenate([pair_a] + ax, axis=0)
    all_b = jnp.concatenate([pair_b] + bz, axis=0)
    az = [along_z(all_a, d) for d in STEPS]
    bx = [along_x(all_b, d) for d in STEPS]

    def a_runs(d):
        return [((4 - e) % 4, 4 - d) for e in (0,) + STEPS]

    def b_runs(d):
        return [(4 - d, (4 - e) % 4) for e in (0,) + STEPS]

    early = [(a, [(4 - d, 0)]) for a, d in zip(ax, STEPS)] + [(b, [(0, 4 - d)]) for b, d in zip(bz, STEPS)]
    state = attend(place, queries, None, own, early)
    state = attend(place, queries, state, None, [(az[i], a_runs(STEPS[i])) for i in (0, 1)])
    state = attend(place, queries, state, None, [(bx[i], b_runs(STEPS[i])) for i in (0, 1)])
    rest = [(az[2], a_runs(STEPS[2])), (bx[2], b_runs(STEPS[2]))]
    heads_out, far = attend(place, queries, state, None, rest, projection)

    far = send(far, lambda z, x, y, h, c: (z, x, y, h, c + 1))
    cross = add(project(heads_out, projection, tp ^ 2), far)
    heads_out, cross = lax.optimization_barrier((heads_out, cross))
    cross = send(cross, lambda z, x, y, h, c: (z, x, y, h + 1, c))
    side = send(project(heads_out, projection, tp ^ 1), lambda z, x, y, h, c: (z, x, y, h, c + 1))
    mine = project(heads_out, projection, tp)
    total = mine.astype(jnp.float32) + side.astype(jnp.float32) + cross.astype(jnp.float32)
    return total.astype(jnp.bfloat16)


def solution(mesh):
    in_specs = (P("seq", "tp"), P("seq", "tp"), P("seq", "tp"), P("tp", None))
    return jax.shard_map(on_device, mesh=mesh, in_specs=in_specs, out_specs=P("seq", "tp"), check_vma=False)
```

```python
import functools

import jax
import jax.numpy as jnp
from jax import lax
from jax.experimental import pallas as pl
from jax.experimental.pallas import tpu as pltpu
from jax.sharding import PartitionSpec as P


NZ, NX, NY, NH, NC = 4, 4, 2, 2, 2
AXES = ("seq", "tp")
HD = 128
UNIT = HD**-0.5 * 1.4426950408889634
LIMIT = 60.0

STEPS = (1, 3, 2)
BLK = 256


def flat(z, x, y, h, c):
    return ((z * NX + x) * NY + y) * NH * NC + h * NC + c


def send(a, move):
    pairs = []
    for z in range(NZ):
        for x in range(NX):
            for y in range(NY):
                for h in range(NH):
                    for c in range(NC):
                        tz, tx, ty, th, tc = move(z, x, y, h, c)
                        tz, tx, ty, th, tc = tz % NZ, tx % NX, ty % NY, th % NH, tc % NC
                        pairs.append((flat(z, x, y, h, c), flat(tz, tx, ty, th, tc)))
    return lax.ppermute(a, AXES, pairs)


def along_x(a, d):
    return send(a, lambda z, x, y, h, c: (z, x + d, y, h, c))


def along_z(a, d):
    return send(a, lambda z, x, y, h, c: (z + d, x, y, h, c))


def exact_fold(h, q_ref, tile, valid, top, acc):
    keys = tile.shape[0]
    q = q_ref[:, pl.ds(pl.multiple_of(h * HD, HD), HD)]
    s = lax.dot_general(q, tile[:, :HD], (((1,), (1,)), ((), ())), preferred_element_type=jnp.float32)
    u = s * UNIT
    if valid is not None:
        u = jnp.where(valid, u, -1e30)
    old = top[h]
    new = jnp.maximum(old, jnp.max(u, axis=1, keepdims=True))
    top[h] = new
    factor = jnp.exp2(old - new)
    p = jnp.exp2(u - jnp.concatenate([new] * (keys // HD), axis=1)).astype(jnp.bfloat16)
    value_mat = jnp.concatenate([tile[:, HD:], jnp.ones((keys, HD), jnp.bfloat16)], axis=1)
    acc[h] = acc[h] * jnp.concatenate([factor, factor], axis=1) + jnp.dot(
        p, value_mat, preferred_element_type=jnp.float32
    )


def fast_fold(q_ref, tile, top, acc, worst):
    keys = tile.shape[0]
    rows = q_ref.shape[0]
    value_mat = jnp.concatenate([tile[:, HD:], jnp.ones((keys, HD), jnp.bfloat16)], axis=1)
    for h in range(acc.shape[0]):
        q = q_ref[:, h * HD : (h + 1) * HD]
        s = lax.dot_general(q, tile[:, :HD], (((1,), (1,)), ((), ())), preferred_element_type=jnp.float32)
        u = s * UNIT - jnp.concatenate([top[h]] * (keys // HD), axis=1)
        high = u[:, :HD]
        for j in range(1, keys // HD):
            high = jnp.maximum(high, u[:, j * HD : (j + 1) * HD])
        p = jnp.exp2(u).astype(jnp.bfloat16)
        acc[h] = acc[h] + jnp.dot(p, value_mat, preferred_element_type=jnp.float32)
        worst = jnp.maximum(worst, jnp.max(high.reshape(rows // 8, 8, HD), axis=0))
    return worst


def fold_own(q_ref, own, y, top, acc):
    rows = q_ref.shape[0]
    top[...] = jnp.full(top.shape, -1e30, jnp.float32)
    acc[...] = jnp.zeros(acc.shape, jnp.float32)
    r = lax.broadcasted_iota(jnp.int32, (rows, 2 * BLK), 0)
    k = lax.broadcasted_iota(jnp.int32, (rows, 2 * BLK), 1)
    position = lax.div(k, 256) * 128 + lax.rem(k, 128)
    position = position + jnp.where(lax.rem(lax.div(k, 128), 2) == 0, 0, jnp.where(y == 0, 256, -256))
    valid = position <= r

    def head(h, carry):
        exact_fold(h, q_ref, own[...], valid, top, acc)
        return carry

    lax.fori_loop(0, acc.shape[0], head, 0, unroll=4)


def own_kernel(place, q_ref, own, top, acc):
    fold_own(q_ref, own, place[2], top, acc)


def step_kernel(place, q_ref, top_in, acc_in, *rest, last, blocks):
    n = len(blocks)
    refs, rest = rest[:n], rest[n:]
    if last:
        w_ref, heads_ref, x_ref, held, top, acc, w_buf, sems = rest
        copies = load_columns(w_ref, place[3], w_buf, sems)
    else:
        top, acc, held = rest
    z, x = place[0], place[1]
    count = jnp.int32(0)
    for ref, sources in zip(refs, blocks):
        for i, (dx, dz) in enumerate(sources):
            needed = lax.rem(z + dz, NZ) * NX + lax.rem(x + dx, NX) < z * NX + x

            @pl.when(needed)
            def _(ref=ref, i=i, at=count):
                held[pl.ds(pl.multiple_of(at * BLK, BLK), BLK), :] = ref[i * BLK : (i + 1) * BLK, :]

            count = count + needed.astype(jnp.int32)

    top[...] = top_in[...]
    acc[...] = acc_in[...]

    def keys_at(i, n):
        return held[pl.ds(pl.multiple_of(i * n, n), n), :]

    def odd(w):
        return fast_fold(q_ref, keys_at(count - 1, BLK), top, acc, w)

    worst = lax.fori_loop(
        0,
        lax.div(count, 2),
        lambda i, w: fast_fold(q_ref, keys_at(i, 2 * BLK), top, acc, w),
        jnp.full((8, HD), -1e30, jnp.float32),
    )
    worst = lax.cond(lax.rem(count, 2) == 1, odd, lambda w: w, worst)

    @pl.when(jnp.max(worst) > LIMIT)
    def _():
        acc[...] = acc_in[...]

        def again(i, carry):
            def head(h, c):
                exact_fold(h, q_ref, keys_at(i, BLK), None, top, acc)
                return c

            return lax.fori_loop(0, acc.shape[0], head, carry)

        lax.fori_loop(0, count, again, 0)

    if last:
        for h in range(acc.shape[0]):
            a = acc[h]
            heads_ref[:, h * HD : (h + 1) * HD] = (a[:, :HD] / a[:, HD:]).astype(jnp.bfloat16)
        multiply_columns(heads_ref, w_buf, copies, x_ref)


WIDTH, CHUNK = 2048, 512


def load_columns(w_ref, part, w_buf, sems):
    copies = []
    for j in range(WIDTH // CHUNK):
        at = pl.multiple_of(part * WIDTH + j * CHUNK, CHUNK)
        copies.append(
            pltpu.make_async_copy(w_ref.at[:, pl.ds(at, CHUNK)], w_buf.at[:, pl.ds(j * CHUNK, CHUNK)], sems.at[j])
        )
        copies[-1].start()
    return copies


def multiply_columns(heads_ref, w_buf, copies, out_ref):
    for j, copy in enumerate(copies):
        copy.wait()
        out_ref[:, j * CHUNK : (j + 1) * CHUNK] = jnp.dot(
            heads_ref[...], w_buf[:, j * CHUNK : (j + 1) * CHUNK], preferred_element_type=jnp.float32
        ).astype(out_ref.dtype)


def project_kernel(part, heads_ref, w_ref, out_ref, w_buf, sems):
    multiply_columns(heads_ref, w_buf, load_columns(w_ref, part[0], w_buf, sems), out_ref)


SMEM = pl.BlockSpec(memory_space=pltpu.SMEM)
VMEM = pl.BlockSpec(memory_space=pltpu.VMEM)
HBM = pl.BlockSpec(memory_space=pltpu.HBM)
W_SCRATCH = [pltpu.VMEM((1024, WIDTH), jnp.bfloat16), pltpu.SemaphoreType.DMA((WIDTH // CHUNK,))]


def cost(blocks, mib):
    n = blocks * 512 * 2048
    return pl.CostEstimate(flops=4 * n * HD, bytes_accessed=mib << 20, transcendentals=n)


def state_of(rows, heads):
    return (
        jax.ShapeDtypeStruct((heads, rows, HD), jnp.float32),
        jax.ShapeDtypeStruct((heads, rows, 2 * HD), jnp.float32),
    )


def attend(place, queries, state, own, operands, projection=None):
    arrays, blocks = [a for a, _ in operands], [b for _, b in operands]
    rows, width = queries.shape
    first, last = own is not None, projection is not None
    shapes = state_of(rows, width // HD)
    in_state = [own] if first else list(state)
    held = [] if first else [pltpu.VMEM((sum(len(b) for b in blocks) * BLK, 2 * HD), jnp.bfloat16)]
    buffers = [pltpu.VMEM(s.shape, s.dtype) for s in shapes]
    out = (jax.ShapeDtypeStruct((rows, width), jnp.bfloat16), jax.ShapeDtypeStruct((rows, WIDTH), jnp.bfloat16))
    return pl.pallas_call(
        own_kernel if first else functools.partial(step_kernel, last=last, blocks=blocks),
        out_shape=out if last else shapes,
        in_specs=[SMEM, VMEM] + [VMEM] * (len(in_state) + len(arrays)) + [HBM] * last,
        out_specs=(VMEM, VMEM),
        scratch_shapes=held + (buffers + W_SCRATCH if last else []),
        compiler_params=pltpu.CompilerParams(vmem_limit_bytes=(45 if last else 20) << 20),
        cost_estimate=cost(1 if first else 4, 8),
        name="attend_last" if last else "attend_own" if first else "attend_step",
    )(place, queries, *in_state, *arrays, *([projection] if last else []))


def pack_kernel(k_ref, v_ref, out_ref):
    out_ref[:, :HD] = k_ref[...]
    out_ref[:, HD:] = v_ref[...]


def pack(key_rows, value_rows):
    return pl.pallas_call(
        pack_kernel,
        out_shape=jax.ShapeDtypeStruct((key_rows.shape[0], 2 * HD), jnp.bfloat16),
        in_specs=[VMEM, VMEM],
        out_specs=VMEM,
        compiler_params=pltpu.CompilerParams(vmem_limit_bytes=4 << 20),
        name="pack",
    )(key_rows, value_rows)


def project(heads_out, projection, part):
    rows = heads_out.shape[0]
    return pl.pallas_call(
        project_kernel,
        out_shape=jax.ShapeDtypeStruct((rows, WIDTH), jnp.bfloat16),
        in_specs=[SMEM, VMEM, HBM],
        out_specs=VMEM,
        scratch_shapes=W_SCRATCH,
        compiler_params=pltpu.CompilerParams(vmem_limit_bytes=50 << 20),
        cost_estimate=pl.CostEstimate(flops=2 * rows * 1024 * WIDTH, bytes_accessed=6 << 20, transcendentals=0),
        name="project",
    )(part.reshape(1), heads_out, projection)


def add(a, b):
    return (a.astype(jnp.float32) + b.astype(jnp.float32)).astype(jnp.bfloat16)


def on_device(queries, key_rows, value_rows, projection):
    seq = lax.axis_index("seq").astype(jnp.int32)
    tp = lax.axis_index("tp").astype(jnp.int32)
    place = jnp.stack([seq // (NX * NY), (seq // NY) % NX, seq % NY, tp ^ 3])

    both = pack(key_rows, value_rows)
    near = send(both, lambda z, x, y, h, c: (z, x, y + 1, h, c))
    pair_a = jnp.concatenate([both[:128], near[:128]], axis=0)
    pair_b = jnp.concatenate([both[128:], near[128:]], axis=0)
    own = jnp.concatenate([pair_a, pair_b], axis=0)
    ax = [along_x(pair_a, d) for d in STEPS]
    bz = [along_z(pair_b, d) for d in STEPS]
    state = attend(place, queries, None, own, [])
    ax, bz, state = lax.optimization_barrier((ax, bz, state))
    all_a = jnp.concatenate([pair_a] + ax, axis=0)
    all_b = jnp.concatenate([pair_b] + bz, axis=0)

    def a_runs(d):
        return [((4 - e) % 4, 4 - d) for e in (0,) + STEPS]

    def b_runs(d):
        return [(4 - d, (4 - e) % 4) for e in (0,) + STEPS]

    az = [along_z(all_a, d) for d in STEPS[:2]]
    bx = [along_x(all_b, d) for d in STEPS[:2]]
    early = [(a, [(4 - d, 0)]) for a, d in zip(ax, STEPS)] + [(b, [(0, 4 - d)]) for b, d in zip(bz, STEPS)]
    state = attend(place, queries, state, None, early)
    az, bx, all_a, all_b, state = lax.optimization_barrier((az, bx, all_a, all_b, state))
    az.append(along_z(all_a, STEPS[2]))
    bx.append(along_x(all_b, STEPS[2]))
    state = attend(place, queries, state, None, [(az[i], a_runs(STEPS[i])) for i in (0, 1)])
    state = attend(place, queries, state, None, [(bx[i], b_runs(STEPS[i])) for i in (0, 1)])
    rest = [(az[2], a_runs(STEPS[2])), (bx[2], b_runs(STEPS[2]))]
    heads_out, far = attend(place, queries, state, None, rest, projection)

    far = send(far, lambda z, x, y, h, c: (z, x, y, h, c + 1))
    cross = add(project(heads_out, projection, tp ^ 2), far)
    heads_out, cross = lax.optimization_barrier((heads_out, cross))
    cross = send(cross, lambda z, x, y, h, c: (z, x, y, h + 1, c))
    side = project(heads_out, projection, tp ^ 1)
    side = send(side, lambda z, x, y, h, c: (z, x, y, h, c + 1))
    mine = project(heads_out, projection, tp)
    total = mine.astype(jnp.float32) + side.astype(jnp.float32) + cross.astype(jnp.float32)
    return total.astype(jnp.bfloat16)


def solution(mesh):
    in_specs = (P("seq", "tp"), P("seq", "tp"), P("seq", "tp"), P("tp", None))
    return jax.shard_map(on_device, mesh=mesh, in_specs=in_specs, out_specs=P("seq", "tp"), check_vma=False)
```

```python
import functools

import jax
import jax.numpy as jnp
from jax import lax
from jax.experimental import pallas as pl
from jax.experimental.pallas import tpu as pltpu
from jax.sharding import PartitionSpec as P


NZ, NX, NY, NH, NC = 4, 4, 2, 2, 2
AXES = ("seq", "tp")
HD = 128
UNIT = HD**-0.5 * 1.4426950408889634
LIMIT = 60.0

STEPS = (1, 3, 2)
BLK = 256


def flat(z, x, y, h, c):
    return ((z * NX + x) * NY + y) * NH * NC + h * NC + c


def send(a, move):
    pairs = []
    for z in range(NZ):
        for x in range(NX):
            for y in range(NY):
                for h in range(NH):
                    for c in range(NC):
                        tz, tx, ty, th, tc = move(z, x, y, h, c)
                        tz, tx, ty, th, tc = tz % NZ, tx % NX, ty % NY, th % NH, tc % NC
                        pairs.append((flat(z, x, y, h, c), flat(tz, tx, ty, th, tc)))
    return lax.ppermute(a, AXES, pairs)


def along(a, d, second):
    def move(z, x, y, h, c):
        return (z, x + d, y, h, c) if (c == 0) != second else (z + d, x, y, h, c)

    return send(a, move)


def exact_fold(h, q_ref, tile, valid, top, acc):
    keys = tile.shape[0]
    q = q_ref[:, pl.ds(pl.multiple_of(h * HD, HD), HD)]
    s = lax.dot_general(q, tile[:, :HD], (((1,), (1,)), ((), ())), preferred_element_type=jnp.float32)
    u = s * UNIT
    if valid is not None:
        u = jnp.where(valid, u, -1e30)
    old = top[h]
    new = jnp.maximum(old, jnp.max(u, axis=1, keepdims=True))
    top[h] = new
    factor = jnp.exp2(old - new)
    p = jnp.exp2(u - jnp.concatenate([new] * (keys // HD), axis=1)).astype(jnp.bfloat16)
    value_mat = jnp.concatenate([tile[:, HD:], jnp.ones((keys, HD), jnp.bfloat16)], axis=1)
    acc[h] = acc[h] * jnp.concatenate([factor, factor], axis=1) + jnp.dot(
        p, value_mat, preferred_element_type=jnp.float32
    )


def fast_fold(q_ref, tile, top, acc, worst):
    keys = tile.shape[0]
    rows = q_ref.shape[0]
    value_mat = jnp.concatenate([tile[:, HD:], jnp.ones((keys, HD), jnp.bfloat16)], axis=1)
    for h in range(acc.shape[0]):
        q = q_ref[:, h * HD : (h + 1) * HD]
        s = lax.dot_general(q, tile[:, :HD], (((1,), (1,)), ((), ())), preferred_element_type=jnp.float32)
        u = s * UNIT - jnp.concatenate([top[h]] * (keys // HD), axis=1)
        high = u[:, :HD]
        for j in range(1, keys // HD):
            high = jnp.maximum(high, u[:, j * HD : (j + 1) * HD])
        p = jnp.exp2(u).astype(jnp.bfloat16)
        acc[h] = acc[h] + jnp.dot(p, value_mat, preferred_element_type=jnp.float32)
        worst = jnp.maximum(worst, jnp.max(high.reshape(rows // 8, 8, HD), axis=0))
    return worst


def fold_own(q_ref, own, y, top, acc):
    rows = q_ref.shape[0]
    top[...] = jnp.full(top.shape, -1e30, jnp.float32)
    acc[...] = jnp.zeros(acc.shape, jnp.float32)
    r = lax.broadcasted_iota(jnp.int32, (rows, 2 * BLK), 0)
    k = lax.broadcasted_iota(jnp.int32, (rows, 2 * BLK), 1)
    position = lax.div(k, 256) * 128 + lax.rem(k, 128)
    position = position + jnp.where(lax.rem(lax.div(k, 128), 2) == 0, 0, jnp.where(y == 0, 256, -256))
    valid = position <= r

    def head(h, carry):
        exact_fold(h, q_ref, own[...], valid, top, acc)
        return carry

    lax.fori_loop(0, acc.shape[0], head, 0, unroll=4)


def own_kernel(place, q_ref, own, top, acc):
    fold_own(q_ref, own, place[2], top, acc)


def step_kernel(place, q_ref, top_in, acc_in, *rest, last, blocks):
    n = len(blocks)
    refs, rest = rest[:n], rest[n:]
    if last:
        w_ref, heads_ref, x_ref, held, top, acc, w_buf, sems = rest
        copies = load_columns(w_ref, place[3], w_buf, sems)
    else:
        top, acc, held = rest
    z, x = place[0], place[1]
    count = jnp.int32(0)
    for ref, sources in zip(refs, blocks):
        for i, (du, dv) in enumerate(sources):
            dx, dz = jnp.where(place[4] == 0, du, dv), jnp.where(place[4] == 0, dv, du)
            needed = lax.rem(z + dz, NZ) * NX + lax.rem(x + dx, NX) < z * NX + x

            @pl.when(needed)
            def _(ref=ref, i=i, at=count):
                held[pl.ds(pl.multiple_of(at * BLK, BLK), BLK), :] = ref[i * BLK : (i + 1) * BLK, :]

            count = count + needed.astype(jnp.int32)

    top[...] = top_in[...]
    acc[...] = acc_in[...]

    def keys_at(i, n):
        return held[pl.ds(pl.multiple_of(i * n, n), n), :]

    def odd(w):
        return fast_fold(q_ref, keys_at(count - 1, BLK), top, acc, w)

    worst = lax.fori_loop(
        0,
        lax.div(count, 2),
        lambda i, w: fast_fold(q_ref, keys_at(i, 2 * BLK), top, acc, w),
        jnp.full((8, HD), -1e30, jnp.float32),
    )
    worst = lax.cond(lax.rem(count, 2) == 1, odd, lambda w: w, worst)

    @pl.when(jnp.max(worst) > LIMIT)
    def _():
        acc[...] = acc_in[...]

        def again(i, carry):
            def head(h, c):
                exact_fold(h, q_ref, keys_at(i, BLK), None, top, acc)
                return c

            return lax.fori_loop(0, acc.shape[0], head, carry)

        lax.fori_loop(0, count, again, 0)

    if last:
        for h in range(acc.shape[0]):
            a = acc[h]
            heads_ref[:, h * HD : (h + 1) * HD] = (a[:, :HD] / a[:, HD:]).astype(jnp.bfloat16)
        multiply_columns(heads_ref, w_buf, copies, x_ref)


WIDTH, CHUNK = 2048, 512


def load_columns(w_ref, part, w_buf, sems):
    copies = []
    for j in range(WIDTH // CHUNK):
        at = pl.multiple_of(part * WIDTH + j * CHUNK, CHUNK)
        copies.append(
            pltpu.make_async_copy(w_ref.at[:, pl.ds(at, CHUNK)], w_buf.at[:, pl.ds(j * CHUNK, CHUNK)], sems.at[j])
        )
        copies[-1].start()
    return copies


def multiply_columns(heads_ref, w_buf, copies, out_ref):
    for j, copy in enumerate(copies):
        copy.wait()
        out_ref[:, j * CHUNK : (j + 1) * CHUNK] = jnp.dot(
            heads_ref[...], w_buf[:, j * CHUNK : (j + 1) * CHUNK], preferred_element_type=jnp.float32
        ).astype(out_ref.dtype)


def project_kernel(part, heads_ref, w_ref, out_ref, w_buf, sems):
    multiply_columns(heads_ref, w_buf, load_columns(w_ref, part[0], w_buf, sems), out_ref)


SMEM = pl.BlockSpec(memory_space=pltpu.SMEM)
VMEM = pl.BlockSpec(memory_space=pltpu.VMEM)
HBM = pl.BlockSpec(memory_space=pltpu.HBM)
W_SCRATCH = [pltpu.VMEM((1024, WIDTH), jnp.bfloat16), pltpu.SemaphoreType.DMA((WIDTH // CHUNK,))]


def cost(blocks, mib):
    n = blocks * 512 * 2048
    return pl.CostEstimate(flops=4 * n * HD, bytes_accessed=mib << 20, transcendentals=n)


def state_of(rows, heads):
    return (
        jax.ShapeDtypeStruct((heads, rows, HD), jnp.float32),
        jax.ShapeDtypeStruct((heads, rows, 2 * HD), jnp.float32),
    )


def attend(place, queries, state, own, operands, projection=None):
    arrays, blocks = [a for a, _ in operands], [b for _, b in operands]
    rows, width = queries.shape
    first, last = own is not None, projection is not None
    shapes = state_of(rows, width // HD)
    in_state = [own] if first else list(state)
    held = [] if first else [pltpu.VMEM((sum(len(b) for b in blocks) * BLK, 2 * HD), jnp.bfloat16)]
    buffers = [pltpu.VMEM(s.shape, s.dtype) for s in shapes]
    out = (jax.ShapeDtypeStruct((rows, width), jnp.bfloat16), jax.ShapeDtypeStruct((rows, WIDTH), jnp.bfloat16))
    return pl.pallas_call(
        own_kernel if first else functools.partial(step_kernel, last=last, blocks=blocks),
        out_shape=out if last else shapes,
        in_specs=[SMEM, VMEM] + [VMEM] * (len(in_state) + len(arrays)) + [HBM] * last,
        out_specs=(VMEM, VMEM),
        scratch_shapes=held + (buffers + W_SCRATCH if last else []),
        compiler_params=pltpu.CompilerParams(vmem_limit_bytes=(45 if last else 20) << 20),
        cost_estimate=cost(1 if first else 4, 8),
        name="attend_last" if last else "attend_own" if first else "attend_step",
    )(place, queries, *in_state, *arrays, *([projection] if last else []))


def pack_kernel(k_ref, v_ref, out_ref):
    out_ref[:, :HD] = k_ref[...]
    out_ref[:, HD:] = v_ref[...]


def pack(key_rows, value_rows):
    return pl.pallas_call(
        pack_kernel,
        out_shape=jax.ShapeDtypeStruct((key_rows.shape[0], 2 * HD), jnp.bfloat16),
        in_specs=[VMEM, VMEM],
        out_specs=VMEM,
        compiler_params=pltpu.CompilerParams(vmem_limit_bytes=4 << 20),
        name="pack",
    )(key_rows, value_rows)


def project(heads_out, projection, part):
    rows = heads_out.shape[0]
    return pl.pallas_call(
        project_kernel,
        out_shape=jax.ShapeDtypeStruct((rows, WIDTH), jnp.bfloat16),
        in_specs=[SMEM, VMEM, HBM],
        out_specs=VMEM,
        scratch_shapes=W_SCRATCH,
        compiler_params=pltpu.CompilerParams(vmem_limit_bytes=50 << 20),
        cost_estimate=pl.CostEstimate(flops=2 * rows * 1024 * WIDTH, bytes_accessed=6 << 20, transcendentals=0),
        name="project",
    )(part.reshape(1), heads_out, projection)


def add(a, b):
    return (a.astype(jnp.float32) + b.astype(jnp.float32)).astype(jnp.bfloat16)


def on_device(queries, key_rows, value_rows, projection):
    seq = lax.axis_index("seq").astype(jnp.int32)
    tp = lax.axis_index("tp").astype(jnp.int32)
    place = jnp.stack([seq // (NX * NY), (seq // NY) % NX, seq % NY, tp ^ 3, tp % NC])

    both = pack(key_rows, value_rows)
    near = send(both, lambda z, x, y, h, c: (z, x, y + 1, h, c))
    pair_a = jnp.concatenate([both[:128], near[:128]], axis=0)
    pair_b = jnp.concatenate([both[128:], near[128:]], axis=0)
    own = jnp.concatenate([pair_a, pair_b], axis=0)
    first_a = [along(pair_a, d, False) for d in STEPS]
    first_b = [along(pair_b, d, True) for d in STEPS]
    state = attend(place, queries, None, own, [])
    first_a, first_b, state = lax.optimization_barrier((first_a, first_b, state))
    all_a = jnp.concatenate([pair_a] + first_a, axis=0)
    all_b = jnp.concatenate([pair_b] + first_b, axis=0)

    def runs(d, a):
        return [((4 - e) % 4, 4 - d) if a else (4 - d, (4 - e) % 4) for e in (0,) + STEPS]

    near_a = [(along(all_a, d, True), runs(d, True)) for d in STEPS[:2]]
    near_b = [(along(all_b, d, False), runs(d, False)) for d in STEPS[:2]]
    early = [(a, [(4 - d, 0)]) for a, d in zip(first_a, STEPS)] + [(b, [(0, 4 - d)]) for b, d in zip(first_b, STEPS)]
    state = attend(place, queries, state, None, early)
    arrays, all_a, state = lax.optimization_barrier(([a for a, _ in near_a], all_a, state))
    far_a = along(all_a, STEPS[2], True)
    state = attend(place, queries, state, None, [(a, r) for a, (_, r) in zip(arrays, near_a)])
    arrays, all_b, state = lax.optimization_barrier(([b for b, _ in near_b], all_b, state))
    far_b = along(all_b, STEPS[2], False)
    state = attend(place, queries, state, None, [(b, r) for b, (_, r) in zip(arrays, near_b)])
    rest = [(far_a, runs(STEPS[2], True)), (far_b, runs(STEPS[2], False))]
    heads_out, far = attend(place, queries, state, None, rest, projection)

    far = send(far, lambda z, x, y, h, c: (z, x, y, h, c + 1))
    cross = add(project(heads_out, projection, tp ^ 2), far)
    heads_out, cross = lax.optimization_barrier((heads_out, cross))
    cross = send(cross, lambda z, x, y, h, c: (z, x, y, h + 1, c))
    side = project(heads_out, projection, tp ^ 1)
    side = send(side, lambda z, x, y, h, c: (z, x, y, h, c + 1))
    mine = project(heads_out, projection, tp)
    total = mine.astype(jnp.float32) + side.astype(jnp.float32) + cross.astype(jnp.float32)
    return total.astype(jnp.bfloat16)


def solution(mesh):
    in_specs = (P("seq", "tp"), P("seq", "tp"), P("seq", "tp"), P("tp", None))
    return jax.shard_map(on_device, mesh=mesh, in_specs=in_specs, out_specs=P("seq", "tp"), check_vma=False)
```

```python
import functools

import jax
import jax.numpy as jnp
from jax import lax
from jax.experimental import pallas as pl
from jax.experimental.pallas import tpu as pltpu
from jax.sharding import PartitionSpec as P


NZ, NX, NY, NH, NC = 4, 4, 2, 2, 2
AXES = ("seq", "tp")
HD = 128
UNIT = HD**-0.5 * 1.4426950408889634
LIMIT = 60.0

STEPS = (1, 3, 2)
BLK = 512


def flat(z, x, y, h, c):
    return ((z * NX + x) * NY + y) * NH * NC + h * NC + c


def send(a, move):
    pairs = []
    for z in range(NZ):
        for x in range(NX):
            for y in range(NY):
                for h in range(NH):
                    for c in range(NC):
                        tz, tx, ty, th, tc = move(z, x, y, h, c)
                        tz, tx, ty, th, tc = tz % NZ, tx % NX, ty % NY, th % NH, tc % NC
                        pairs.append((flat(z, x, y, h, c), flat(tz, tx, ty, th, tc)))
    return lax.ppermute(a, AXES, pairs)


def along(a, d, second):
    def move(z, x, y, h, c):
        return (z, x + d, y, h, c) if (c == 0) != second else (z + d, x, y, h, c)

    return send(a, move)


def exact_fold(h, q_ref, tile, valid, top, acc):
    keys = tile.shape[0]
    q = q_ref[:, pl.ds(pl.multiple_of(h * HD, HD), HD)]
    s = lax.dot_general(q, tile[:, :HD], (((1,), (1,)), ((), ())), preferred_element_type=jnp.float32)
    u = s * UNIT
    if valid is not None:
        u = jnp.where(valid, u, -1e30)
    old = top[h]
    new = jnp.maximum(old, jnp.max(u, axis=1, keepdims=True))
    top[h] = new
    factor = jnp.exp2(old - new)
    p = jnp.exp2(u - jnp.concatenate([new] * (keys // HD), axis=1)).astype(jnp.bfloat16)
    value_mat = jnp.concatenate([tile[:, HD:], jnp.ones((keys, HD), jnp.bfloat16)], axis=1)
    acc[h] = acc[h] * jnp.concatenate([factor, factor], axis=1) + jnp.dot(
        p, value_mat, preferred_element_type=jnp.float32
    )


def fast_fold(q_ref, tile, top, acc, worst):
    keys = tile.shape[0]
    rows = q_ref.shape[0]
    value_mat = jnp.concatenate([tile[:, HD:], jnp.ones((keys, HD), jnp.bfloat16)], axis=1)
    for h in range(acc.shape[0]):
        q = q_ref[:, h * HD : (h + 1) * HD]
        s = lax.dot_general(q, tile[:, :HD], (((1,), (1,)), ((), ())), preferred_element_type=jnp.float32)
        u = s * UNIT - jnp.concatenate([top[h]] * (keys // HD), axis=1)
        high = u[:, :HD]
        for j in range(1, keys // HD):
            high = jnp.maximum(high, u[:, j * HD : (j + 1) * HD])
        p = jnp.exp2(u).astype(jnp.bfloat16)
        acc[h] = acc[h] + jnp.dot(p, value_mat, preferred_element_type=jnp.float32)
        worst = jnp.maximum(worst, jnp.max(high.reshape(rows // 8, 8, HD), axis=0))
    return worst


def fold_own(q_ref, own, y, top, acc):
    rows = q_ref.shape[0]
    top[...] = jnp.full(top.shape, -1e30, jnp.float32)
    acc[...] = jnp.zeros(acc.shape, jnp.float32)
    r = lax.broadcasted_iota(jnp.int32, (rows, BLK), 0)
    k = lax.broadcasted_iota(jnp.int32, (rows, BLK), 1)
    valid = jnp.where(k < 256, k, k + jnp.where(y == 0, 0, -512)) <= r

    def head(h, carry):
        exact_fold(h, q_ref, own[...], valid, top, acc)
        return carry

    lax.fori_loop(0, acc.shape[0], head, 0, unroll=4)


def own_kernel(place, q_ref, own, top, acc):
    fold_own(q_ref, own, place[2], top, acc)


def step_kernel(place, q_ref, top_in, acc_in, *rest, last, blocks):
    n = len(blocks)
    refs, rest = rest[:n], rest[n:]
    if last:
        w_ref, heads_ref, x_ref, held, top, acc, w_buf, sems = rest
        copies = load_columns(w_ref, place[3], w_buf, sems)
    else:
        top, acc, held = rest
    z, x = place[0], place[1]
    count = jnp.int32(0)
    for ref, sources in zip(refs, blocks):
        for i, (du, dv) in enumerate(sources):
            dx, dz = jnp.where(place[4] == 0, du, dv), jnp.where(place[4] == 0, dv, du)
            needed = lax.rem(z + dz, NZ) * NX + lax.rem(x + dx, NX) < z * NX + x

            @pl.when(needed)
            def _(ref=ref, i=i, at=count):
                held[pl.ds(pl.multiple_of(at * BLK, BLK), BLK), :] = ref[i * BLK : (i + 1) * BLK, :]

            count = count + needed.astype(jnp.int32)

    top[...] = top_in[...]
    acc[...] = acc_in[...]

    def keys_at(i):
        return held[pl.ds(pl.multiple_of(i * BLK, BLK), BLK), :]

    worst = lax.fori_loop(
        0,
        count,
        lambda i, w: fast_fold(q_ref, keys_at(i), top, acc, w),
        jnp.full((8, HD), -1e30, jnp.float32),
    )

    @pl.when(jnp.max(worst) > LIMIT)
    def _():
        acc[...] = acc_in[...]

        def again(i, carry):
            def head(h, c):
                exact_fold(h, q_ref, keys_at(i), None, top, acc)
                return c

            return lax.fori_loop(0, acc.shape[0], head, carry)

        lax.fori_loop(0, count, again, 0)

    if last:
        for h in range(acc.shape[0]):
            a = acc[h]
            heads_ref[:, h * HD : (h + 1) * HD] = (a[:, :HD] / a[:, HD:]).astype(jnp.bfloat16)
        multiply_columns(heads_ref, w_buf, copies, x_ref)


WIDTH, CHUNK = 2048, 512


def load_columns(w_ref, part, w_buf, sems):
    copies = []
    for j in range(WIDTH // CHUNK):
        at = pl.multiple_of(part * WIDTH + j * CHUNK, CHUNK)
        copies.append(
            pltpu.make_async_copy(w_ref.at[:, pl.ds(at, CHUNK)], w_buf.at[:, pl.ds(j * CHUNK, CHUNK)], sems.at[j])
        )
        copies[-1].start()
    return copies


def multiply_columns(heads_ref, w_buf, copies, out_ref):
    for j, copy in enumerate(copies):
        copy.wait()
        out_ref[:, j * CHUNK : (j + 1) * CHUNK] = jnp.dot(
            heads_ref[...], w_buf[:, j * CHUNK : (j + 1) * CHUNK], preferred_element_type=jnp.float32
        ).astype(out_ref.dtype)


def project_kernel(part, heads_ref, w_ref, out_ref, w_buf, sems):
    multiply_columns(heads_ref, w_buf, load_columns(w_ref, part[0], w_buf, sems), out_ref)


SMEM = pl.BlockSpec(memory_space=pltpu.SMEM)
VMEM = pl.BlockSpec(memory_space=pltpu.VMEM)
HBM = pl.BlockSpec(memory_space=pltpu.HBM)
W_SCRATCH = [pltpu.VMEM((1024, WIDTH), jnp.bfloat16), pltpu.SemaphoreType.DMA((WIDTH // CHUNK,))]


def cost(blocks, mib):
    n = blocks * BLK * 2048
    return pl.CostEstimate(flops=4 * n * HD, bytes_accessed=mib << 20, transcendentals=n)


def state_of(rows, heads):
    return (
        jax.ShapeDtypeStruct((heads, rows, HD), jnp.float32),
        jax.ShapeDtypeStruct((heads, rows, 2 * HD), jnp.float32),
    )


def attend(place, queries, state, own, operands, projection=None):
    arrays, blocks = [a for a, _ in operands], [b for _, b in operands]
    rows, width = queries.shape
    first, last = own is not None, projection is not None
    shapes = state_of(rows, width // HD)
    in_state = [own] if first else list(state)
    held = [] if first else [pltpu.VMEM((sum(len(b) for b in blocks) * BLK, 2 * HD), jnp.bfloat16)]
    buffers = [pltpu.VMEM(s.shape, s.dtype) for s in shapes]
    out = (jax.ShapeDtypeStruct((rows, width), jnp.bfloat16), jax.ShapeDtypeStruct((rows, WIDTH), jnp.bfloat16))
    return pl.pallas_call(
        own_kernel if first else functools.partial(step_kernel, last=last, blocks=blocks),
        out_shape=out if last else shapes,
        in_specs=[SMEM, VMEM] + [VMEM] * (len(in_state) + len(arrays)) + [HBM] * last,
        out_specs=(VMEM, VMEM),
        scratch_shapes=held + (buffers + W_SCRATCH if last else []),
        compiler_params=pltpu.CompilerParams(vmem_limit_bytes=(45 if last else 20) << 20),
        cost_estimate=cost(1 if first else sum(len(b) for b in blocks), 8),
        name="attend_last" if last else "attend_own" if first else "attend_step",
    )(place, queries, *in_state, *arrays, *([projection] if last else []))


def pack_kernel(k_ref, v_ref, out_ref):
    out_ref[:, :HD] = k_ref[...]
    out_ref[:, HD:] = v_ref[...]


def pack(key_rows, value_rows):
    return pl.pallas_call(
        pack_kernel,
        out_shape=jax.ShapeDtypeStruct((key_rows.shape[0], 2 * HD), jnp.bfloat16),
        in_specs=[VMEM, VMEM],
        out_specs=VMEM,
        compiler_params=pltpu.CompilerParams(vmem_limit_bytes=4 << 20),
        name="pack",
    )(key_rows, value_rows)


def project(heads_out, projection, part):
    rows = heads_out.shape[0]
    return pl.pallas_call(
        project_kernel,
        out_shape=jax.ShapeDtypeStruct((rows, WIDTH), jnp.bfloat16),
        in_specs=[SMEM, VMEM, HBM],
        out_specs=VMEM,
        scratch_shapes=W_SCRATCH,
        compiler_params=pltpu.CompilerParams(vmem_limit_bytes=50 << 20),
        cost_estimate=pl.CostEstimate(flops=2 * rows * 1024 * WIDTH, bytes_accessed=6 << 20, transcendentals=0),
        name="project",
    )(part.reshape(1), heads_out, projection)


def add(a, b):
    return (a.astype(jnp.float32) + b.astype(jnp.float32)).astype(jnp.bfloat16)


def on_device(queries, key_rows, value_rows, projection):
    seq = lax.axis_index("seq").astype(jnp.int32)
    tp = lax.axis_index("tp").astype(jnp.int32)
    place = jnp.stack([seq // (NX * NY), (seq // NY) % NX, seq % NY, tp ^ 3, tp % NC])

    both = pack(key_rows, value_rows)
    near = send(both, lambda z, x, y, h, c: (z, x, y + 1, h, c))
    own = jnp.concatenate([both, near], axis=0)
    first = [along(own, d, False) for d in STEPS]
    state = attend(place, queries, None, own, [])
    first, state = lax.optimization_barrier((first, state))
    line = jnp.concatenate([own] + first, axis=0)

    def runs(d):
        return [((4 - e) % 4, 4 - d) for e in (0,) + STEPS]

    lines = [along(line, d, True) for d in STEPS[:2]]
    state = attend(place, queries, state, None, [(a, [(4 - d, 0)]) for a, d in zip(first, STEPS)])
    lines, line, state = lax.optimization_barrier((lines, line, state))
    last = along(line, STEPS[2], True)
    state = attend(place, queries, state, None, [(a, runs(d)) for a, d in zip(lines, STEPS)])
    heads_out, far = attend(place, queries, state, None, [(last, runs(STEPS[2]))], projection)

    far = send(far, lambda z, x, y, h, c: (z, x, y, h, c + 1))
    cross = add(project(heads_out, projection, tp ^ 2), far)
    heads_out, cross = lax.optimization_barrier((heads_out, cross))
    cross = send(cross, lambda z, x, y, h, c: (z, x, y, h + 1, c))
    side = project(heads_out, projection, tp ^ 1)
    side = send(side, lambda z, x, y, h, c: (z, x, y, h, c + 1))
    mine = project(heads_out, projection, tp)
    total = mine.astype(jnp.float32) + side.astype(jnp.float32) + cross.astype(jnp.float32)
    return total.astype(jnp.bfloat16)


def solution(mesh):
    in_specs = (P("seq", "tp"), P("seq", "tp"), P("seq", "tp"), P("tp", None))
    return jax.shard_map(on_device, mesh=mesh, in_specs=in_specs, out_specs=P("seq", "tp"), check_vma=False)
```
